32 devices in a mesh: dom: 4 (over z), col: 8 (over y, x, core).
Axes of the slice: x: 2, y: 2, z: 4, core: 2. Of those that a mesh axis runs over, the one named last changes fastest.
Arguments:
- rhs_interior: bfloat16 [4, 48, 8192], P('dom', 'col'), may hold values from -6 to 6
- interior_inv: bfloat16 [4, 8192, 8192], P('dom', None, 'col'), may hold values from -0.0625 to 0.0625
- coupling: bfloat16 [4, 8192, 768], P('dom', 'col'), may hold values from -0.0625 to 0.0625
- rhs_interface: bfloat16 [48, 8192], P('col', 'dom'), may hold values from -6 to 6
- block_ids: int32 [4, 6], P('dom'), may hold values from 0 to 63, as said below
- interface_inv: bfloat16 [8192, 8192], P('dom', 'col'), may hold values from -0.0625 to 0.0625
Outputs:
- interior_solution: bfloat16 [4, 48, 8192], P('dom', None, 'col')
- interface_solution: bfloat16 [48, 8192], P('col')
The draws below stay inside these ranges and needn't reach their ends.
Inputs may be any that keep to these rules, and one draw needn't show every extreme that they name: `block_ids`: each row names 6 different blocks.
All inputs are finite; a program needn't handle non-finite values.
Results may differ from the reference program's by a relative error of at most 0.025.
Values may be sent and summed in bfloat16 or wider, within the bound.
No kernel may reach another device: no remote copies, remote signals or barrier semaphores. Data moves between devices by JAX's collectives and lax.ppermute only.
A program may use at most 64 MiB of HBM per device.

```python
import jax
import jax.numpy as jnp
from jax import lax

NI = 8192
G = 8192
BS = 128
KB = 6
NSUB = 4
R = 48
LI = 768


def draw_block_ids(key, part):
    keys = jax.random.split(jax.random.fold_in(key, 7), NSUB)
    orders = jax.vmap(lambda single: jax.random.permutation(single, G // BS))(keys)
    return orders[:, :KB].astype(jnp.int32)


def shard_levels(rng, shape, cuts, low, top_value):
    level = 1.0
    for dim, parts in cuts:
        draws = jax.random.uniform(jax.random.fold_in(jax.random.fold_in(rng, 6), dim), (parts,), jnp.float32, low / len(cuts), top_value / len(cuts))
        level = level * jnp.repeat(jnp.exp(draws), shape[dim] // parts).reshape((-1,) + (1,) * (len(shape) - 1 - dim))
    return level


def gaussian(rng, shape, scale, bound, shards=(), held_as=jnp.bfloat16):
    drawn = jax.random.normal(rng, shape, jnp.float32) * scale
    if len(shards) > 0:
        drawn = shard_levels(rng, shape, shards, -0.22, 0.18) * drawn
    return jnp.clip(drawn, min=-bound, max=bound).astype(held_as)


def setup_inputs(seed: int = 0) -> dict:
    arg_keys = jax.random.split(jax.random.key(seed), 7)
    rhs_interior = gaussian(arg_keys[0], (NSUB, R, NI), 1.0, 6.0, ((0, 4), (1, 8)))
    interior_inv = gaussian(arg_keys[1], (NSUB, NI, NI), NI ** -0.5, 0.0625, ((0, 4), (2, 8)))
    coupling = gaussian(arg_keys[2], (NSUB, NI, LI), NI ** -0.5, 0.0625, ((0, 4), (1, 8)))
    rhs_interface = gaussian(arg_keys[3], (R, G), 1.0, 6.0, ((0, 8), (1, 4)))
    block_ids = draw_block_ids(jax.random.fold_in(arg_keys[6], 71), 0)
    interface_inv = gaussian(arg_keys[5], (G, G), G ** -0.5, 0.0625, ((0, 4), (1, 8)))
    return {"rhs_interior": rhs_interior, "interior_inv": interior_inv, "coupling": coupling, "rhs_interface": rhs_interface, "block_ids": block_ids, "interface_inv": interface_inv}


def reference(rhs_interior, interior_inv, coupling, rhs_interface, block_ids, interface_inv):
    nblocks = G // BS
    onehot = (block_ids[:, :, None] == jnp.arange(nblocks, dtype=jnp.int32)[None, None, :]).astype(jnp.float32)

    def forward(running, items):
        rhs_block, inverse, couple, select = items
        step = jnp.dot(rhs_block, inverse, preferred_element_type=jnp.float32).astype(jnp.bfloat16)
        contribution = jnp.dot(step, couple, preferred_element_type=jnp.float32)
        placed = jnp.einsum("kb,rks->rbs", select, contribution.reshape(R, KB, BS)).reshape(R, G)
        return running + placed, None

    summed, unused = lax.scan(forward, jnp.zeros((R, G), jnp.float32), (rhs_interior, interior_inv, coupling, onehot))
    reduced = (rhs_interface.astype(jnp.float32) - summed).astype(jnp.bfloat16)
    interface_solution = jnp.dot(reduced, interface_inv, preferred_element_type=jnp.float32).astype(jnp.bfloat16)
    solution_blocks = interface_solution.astype(jnp.float32).reshape(R, nblocks, BS)

    def backward(items):
        rhs_block, inverse, couple, select = items
        local_solution = jnp.einsum("kb,rbs->rks", select, solution_blocks).reshape(R, LI).astype(jnp.bfloat16)
        correction = jnp.dot(local_solution, couple.T, preferred_element_type=jnp.float32)
        interior_rhs = (rhs_block.astype(jnp.float32) - correction).astype(jnp.bfloat16)
        return jnp.dot(interior_rhs, inverse, preferred_element_type=jnp.float32).astype(jnp.bfloat16)

    interior_solution = lax.map(backward, (rhs_interior, interior_inv, coupling, onehot))
    return interior_solution, interface_solution
```

```python
import jax
import jax.numpy as jnp
from jax import lax
from jax.sharding import PartitionSpec as P


def exchange(value, axis):
    size = lax.axis_size(axis)
    pieces = [value]
    for shift in range(1, size):
        pairs = [(source, (source + shift) % size) for source in range(size)]
        pieces.append(lax.ppermute(value, axis, pairs))
    return pieces


def per_device(rhs_interior, interior_inv, coupling, rhs_interface, block_ids, interface_inv):
    rhs_local = rhs_interior[0]
    inverse = interior_inv[0]
    couple = coupling[0]
    blocks = block_ids[0]
    row_count, interior_count = rhs_local.shape
    block_count = blocks.shape[0]
    block_size = couple.shape[1] // block_count
    col_size = lax.axis_size("col")
    dom_size = lax.axis_size("dom")
    rows = row_count * col_size
    slice_width = rhs_interface.shape[1]
    slice_blocks = slice_width // block_size
    nblocks = slice_blocks * dom_size
    own_columns = couple.shape[0]
    col = lax.axis_index("col")
    dom = lax.axis_index("dom")

    every_blocks = jnp.stack(exchange(blocks, "dom"))
    joined = jnp.concatenate([rhs_local, rhs_interface], axis=1)
    gathered = lax.all_gather(joined, "col", axis=0, tiled=True)
    rhs_all = gathered[:, :interior_count]
    interface_rows = gathered[:, interior_count:]

    step = jnp.dot(rhs_all, inverse, preferred_element_type=jnp.float32).astype(jnp.bfloat16)
    partial = jnp.dot(step, couple, preferred_element_type=jnp.float32).astype(jnp.bfloat16)
    partials = lax.all_gather(partial, "col", axis=0)
    contribution = jnp.sum(partials.astype(jnp.float32), axis=0).astype(jnp.bfloat16)
    contributions = jnp.stack(exchange(contribution, "dom"))
    local_ids = every_blocks - dom * slice_blocks
    onehot = (local_ids[:, :, None] == jnp.arange(slice_blocks, dtype=jnp.int32)).astype(jnp.bfloat16)
    summed = jnp.einsum(
        "dkb,drks->rbs",
        onehot,
        contributions.reshape(dom_size, rows, block_count, block_size),
        preferred_element_type=jnp.float32,
    ).reshape(rows, slice_width)
    reduced = (interface_rows.astype(jnp.float32) - summed).astype(jnp.bfloat16)
    part_solution = jnp.dot(
        reduced, interface_inv, preferred_element_type=jnp.float32
    ).astype(jnp.bfloat16)
    total = sum(piece.astype(jnp.float32) for piece in exchange(part_solution, "dom"))
    every_total = lax.all_gather(total.astype(jnp.bfloat16), "col", axis=1, tiled=True)
    solution = lax.dynamic_slice_in_dim(every_total, col * row_count, row_count, axis=0)
    picks = (blocks[:, None] == jnp.arange(nblocks, dtype=jnp.int32)).astype(jnp.bfloat16)
    local_solution = jnp.einsum(
        "kb,rbs->rks",
        picks,
        every_total.reshape(rows, nblocks, block_size),
        preferred_element_type=jnp.float32,
    ).reshape(rows, block_count * block_size).astype(jnp.bfloat16)
    correction = jnp.einsum("rl,il->ri", local_solution, couple, preferred_element_type=jnp.float32)
    rhs_columns = lax.dynamic_slice_in_dim(rhs_all, col * own_columns, own_columns, axis=1)
    interior_rhs = (rhs_columns.astype(jnp.float32) - correction).astype(jnp.bfloat16)
    result = jnp.dot(
        lax.all_gather(interior_rhs, "col", axis=1, tiled=True),
        inverse,
        preferred_element_type=jnp.float32,
    )
    return (result.astype(jnp.bfloat16)[None], solution)


def solution(mesh):
    placed = (
        P("dom", "col", None),
        P("dom", None, "col"),
        P("dom", "col", None),
        P("col", "dom"),
        P("dom", None),
        P("dom", "col"),
    )
    return jax.shard_map(
        per_device,
        mesh=mesh,
        in_specs=placed,
        out_specs=(P("dom", None, "col"), P("col", None)),
        check_vma=False,
    )
```

```python
import functools

import jax
import jax.numpy as jnp
from jax import lax
from jax.experimental import pallas as pl
from jax.experimental.pallas import tpu as pltpu
from jax.sharding import PartitionSpec as P

LANES = 128
CORES = 2
BF16 = jnp.bfloat16
F32 = jnp.float32
WHOLE = pl.BlockSpec(memory_space=pltpu.VMEM)


def run(kernel, outputs, operands, flops, scratch=(), limit=8):
    return pl.pallas_call(
        kernel,
        out_shape=[jax.ShapeDtypeStruct(shape, BF16) for shape in outputs],
        in_specs=[WHOLE] * len(operands),
        out_specs=[WHOLE] * len(outputs),
        scratch_shapes=list(scratch),
        compiler_params=pltpu.CompilerParams(vmem_limit_bytes=limit * 2**20),
        cost_estimate=pl.CostEstimate(flops=flops, bytes_accessed=2**20, transcendentals=0),
    )(*[pltpu.with_memory_space_constraint(operand, pltpu.VMEM) for operand in operands])


def pairs_of(size, shift, stride=1):
    members = size // stride
    xor = members & (members - 1) == 0
    pairs = []
    for source in range(size):
        unit, rest = divmod(source, stride)
        target = unit ^ shift if xor else (unit + shift) % members
        pairs.append((source, target * stride + rest))
    return pairs


def exchange(value, axis, stride=1):
    size = lax.axis_size(axis)
    return [
        lax.ppermute(value, axis, pairs_of(size, shift, stride))
        for shift in range(1, size // stride)
    ]


def dot(left, right):
    return jnp.dot(left, right, preferred_element_type=F32)


def forward_kernel(half_rows, gathered, inverse, couple, keep, give, rhs):
    slabs, row_count, _ = gathered.shape
    interior = inverse.shape[0]
    order = [slab for core in range(CORES) for slab in range(core, slabs, CORES)]
    for place, slab in enumerate(order):
        rhs[place * row_count : (place + 1) * row_count, :] = gathered[slab, :, :interior]
    step = dot(rhs[...], inverse[...]).astype(BF16)
    part = dot(step, couple[...]).astype(BF16)
    core = lax.rem(lax.axis_index("col"), CORES)

    @pl.when(core == 0)
    def _():
        keep[...] = part[:half_rows]
        give[...] = part[half_rows:]

    @pl.when(core == 1)
    def _():
        keep[...] = part[half_rows:]
        give[...] = part[:half_rows]


def join_kernel(local, interface, out, sems):
    interior = local.shape[1]
    first = pltpu.make_async_copy(local, out.at[:, :interior], sems.at[0])
    second = pltpu.make_async_copy(interface, out.at[:, interior:], sems.at[1])
    first.start()
    second.start()
    first.wait()
    second.wait()


def add_kernel(*refs):
    out = refs[-1]
    total = refs[0][...].astype(F32)
    for ref in refs[1:-1]:
        total = total + ref[...].astype(F32)
    out[...] = total.astype(BF16)


def pack_kernel(block_count, *refs):
    ids, out = refs[-2], refs[-1]
    width = refs[0].shape[1]
    total = refs[0][...].astype(F32)
    for ref in refs[1:-2]:
        total = total + ref[...].astype(F32)
    out[:, :width] = total.astype(BF16)
    out[:, width:] = jnp.broadcast_to(ids[...].astype(F32), (out.shape[0], LANES)).astype(BF16)


def place_kernel(block_count, block_size, gathered, *refs):
    pieces, out = refs[:-1], refs[-1]
    row_count = gathered.shape[1]
    rows, width = out.shape
    interior = gathered.shape[2] - width
    core = lax.rem(lax.axis_index("col"), CORES)
    base = (lax.axis_index("dom") * (width // block_size)).astype(F32)
    span = block_count * block_size
    ids = []
    for piece in pieces:
        tail = piece[:, span:].astype(F32) - base
        for block in range(block_count):
            ids.append(jnp.broadcast_to(tail[:, block : block + 1], (rows, block_size)))
    for target in range(width // block_size):
        lanes = slice(target * block_size, (target + 1) * block_size)
        total = jnp.zeros((rows, block_size), F32)
        for index, name in enumerate(ids):
            piece, block = divmod(index, block_count)
            held = pieces[piece][:, block * block_size : (block + 1) * block_size]
            total = total + jnp.where(name == float(target), held.astype(F32), 0.0)
        source = slice(interior + lanes.start, interior + lanes.stop)
        for chip in range(rows // row_count):
            part = slice(chip * row_count, (chip + 1) * row_count)
            have = gathered[CORES * chip + core, :, source].astype(F32)
            out[part, lanes] = (have - total[part]).astype(BF16)


def interface_kernel(mine, other, inverse, out, reduced):
    core = lax.rem(lax.axis_index("col"), CORES)
    rows = mine.shape[0]

    @pl.when(core == 0)
    def _():
        reduced[:rows] = mine[...]
        reduced[rows:] = other[...]

    @pl.when(core == 1)
    def _():
        reduced[:rows] = other[...]
        reduced[rows:] = mine[...]

    out[...] = dot(reduced[...], inverse[...]).astype(BF16)


def backward_kernel(block_size, ids, total, gathered, couple, out, solution, picked):
    slabs, rows, columns = total.shape
    row_count = gathered.shape[1]
    own_columns = couple.shape[0]
    block_count = couple.shape[1] // block_size
    per_slab = columns // block_size
    col = lax.axis_index("col")
    for block in range(block_count):
        name = ids[0, block]
        slab = lax.div(name, per_slab)
        offset = pl.multiple_of(lax.rem(name, per_slab) * block_size, block_size)
        picked[:, block * block_size : (block + 1) * block_size] = total[slab, :, pl.ds(offset, block_size)]
    row = lax.broadcasted_iota(jnp.int32, (rows, rows), 0)
    place = lax.broadcasted_iota(jnp.int32, (rows, rows), 1)
    owner = lax.div(row, row_count)
    held = (
        lax.rem(owner, CORES) * (rows // CORES)
        + lax.div(owner, CORES) * row_count
        + lax.rem(row, row_count)
    )
    turn = (held == place).astype(F32).astype(BF16)
    local = dot(turn, picked[...]).astype(BF16)
    correction = lax.dot_general(
        local, couple[...], (((1,), (1,)), ((), ())), preferred_element_type=F32
    )
    start = pl.multiple_of(col * own_columns, LANES)
    for slab in range(slabs):
        part = slice(slab * row_count, (slab + 1) * row_count)
        have = gathered[slab, :, pl.ds(start, own_columns)].astype(F32)
        out[part] = (have - correction[part]).astype(BF16)
    first = lax.rem(col, CORES) * (rows // CORES) + lax.div(col, CORES) * row_count
    pick_row = lax.broadcasted_iota(jnp.int32, (8, rows), 0)
    pick_place = lax.broadcasted_iota(jnp.int32, (8, rows), 1)
    pick = (pick_row + first == pick_place).astype(F32).astype(BF16)
    for slab in range(slabs):
        chosen = dot(pick, total[slab])[:row_count]
        solution[:, slab * columns : (slab + 1) * columns] = chosen.astype(BF16)


def last_kernel(every, inverse, out, rhs):
    slabs, rows, columns = every.shape
    for slab in range(slabs):
        rhs[:, slab * columns : (slab + 1) * columns] = every[slab]
    out[...] = dot(rhs[...], inverse[...]).astype(BF16)


def per_device(rhs_interior, interior_inv, coupling, rhs_interface, block_ids, interface_inv):
    rhs_local = rhs_interior[0]
    inverse = interior_inv[0]
    couple = coupling[0]
    row_count, interior = rhs_local.shape
    own_columns, local_count = couple.shape
    block_count = block_ids.shape[1]
    block_size = local_count // block_count
    col_size = lax.axis_size("col")
    rows = row_count * col_size
    half = rows // CORES
    width = rhs_interface.shape[1]
    columns = interface_inv.shape[1]

    joined = pl.pallas_call(
        join_kernel,
        out_shape=jax.ShapeDtypeStruct((row_count, interior + width), BF16),
        in_specs=[pl.BlockSpec(memory_space=pltpu.HBM)] * 2,
        out_specs=WHOLE,
        scratch_shapes=[pltpu.SemaphoreType.DMA((2,))],
        compiler_params=pltpu.CompilerParams(vmem_limit_bytes=8 * 2**20),
        cost_estimate=pl.CostEstimate(
            flops=64 * rows * columns * interior, bytes_accessed=2**20, transcendentals=0
        ),
    )(
        pltpu.with_memory_space_constraint(rhs_local, pltpu.HBM),
        pltpu.with_memory_space_constraint(rhs_interface, pltpu.HBM),
    )
    gathered = lax.all_gather(joined, "col", axis=0)
    ids_row = jnp.pad(block_ids, ((0, 0), (0, LANES - block_count)))

    keep, give = run(
        functools.partial(forward_kernel, half),
        [(half, local_count)] * 2,
        [gathered, inverse, couple],
        2 * rows * own_columns * (interior + local_count),
        [pltpu.VMEM((rows, interior), BF16)],
        limit=12,
    )
    other = lax.ppermute(give, "col", [(source, source ^ 1) for source in range(col_size)])
    (pair,) = run(add_kernel, [(half, local_count)], [keep, other], half * local_count)
    (packed,) = run(
        functools.partial(pack_kernel, block_count),
        [(half, local_count + LANES)],
        [pair, *exchange(pair, "col", CORES), ids_row],
        half * local_count,
    )
    (reduced,) = run(
        functools.partial(place_kernel, block_count, block_size),
        [(half, width)],
        [gathered, packed, *exchange(packed, "dom")],
        rows * width * 64,
        limit=16,
    )
    reduced_other = lax.ppermute(reduced, "col", [(source, source ^ 1) for source in range(col_size)])
    (part_solution,) = run(
        interface_kernel,
        [(rows, columns)],
        [reduced, reduced_other, interface_inv],
        2 * rows * width * columns,
        [pltpu.VMEM((rows, width), BF16)],
    )
    (total,) = run(
        add_kernel,
        [(rows, columns)],
        [part_solution, *exchange(part_solution, "dom")],
        rows * columns,
    )
    every_total = lax.all_gather(total, "col", axis=0)
    interior_rhs, solution = pl.pallas_call(
        functools.partial(backward_kernel, block_size),
        out_shape=[
            jax.ShapeDtypeStruct((rows, own_columns), BF16),
            jax.ShapeDtypeStruct((row_count, columns * col_size), BF16),
        ],
        in_specs=[pl.BlockSpec(memory_space=pltpu.SMEM)] + [WHOLE] * 3,
        out_specs=[WHOLE] * 2,
        scratch_shapes=[pltpu.VMEM((rows, local_count), BF16)],
        compiler_params=pltpu.CompilerParams(vmem_limit_bytes=8 * 2**20),
        cost_estimate=pl.CostEstimate(
            flops=2 * rows * own_columns * local_count, bytes_accessed=2**20, transcendentals=0
        ),
    )(
        block_ids,
        pltpu.with_memory_space_constraint(every_total, pltpu.VMEM),
        pltpu.with_memory_space_constraint(gathered, pltpu.VMEM),
        pltpu.with_memory_space_constraint(couple, pltpu.VMEM),
    )
    every_rhs = lax.all_gather(interior_rhs, "col", axis=0)
    (result,) = run(
        last_kernel,
        [(rows, own_columns)],
        [every_rhs, inverse],
        2 * rows * own_columns * interior,
        [pltpu.VMEM((rows, interior), BF16)],
    )
    return (result[None], solution)


def solution(mesh):
    placed = (
        P("dom", "col", None),
        P("dom", None, "col"),
        P("dom", "col", None),
        P("col", "dom"),
        P("dom", None),
        P("dom", "col"),
    )
    return jax.shard_map(
        per_device,
        mesh=mesh,
        in_specs=placed,
        out_specs=(P("dom", None, "col"), P("col", None)),
        check_vma=False,
    )
```

```python
import functools

import jax
import jax.numpy as jnp
from jax import lax
from jax.experimental import pallas as pl
from jax.experimental.pallas import tpu as pltpu
from jax.sharding import PartitionSpec as P


LANES = 128
CORES = 2
BF16 = jnp.bfloat16
F32 = jnp.float32
WHOLE = pl.BlockSpec(memory_space=pltpu.VMEM)


def run(kernel, outputs, operands, flops, scratch=(), limit=8):
    return pl.pallas_call(
        kernel,
        out_shape=[jax.ShapeDtypeStruct(shape, BF16) for shape in outputs],
        in_specs=[WHOLE] * len(operands),
        out_specs=[WHOLE] * len(outputs),
        scratch_shapes=list(scratch),
        compiler_params=pltpu.CompilerParams(vmem_limit_bytes=limit * 2**20),
        cost_estimate=pl.CostEstimate(flops=flops, bytes_accessed=2**20, transcendentals=0),
    )(*[pltpu.with_memory_space_constraint(operand, pltpu.VMEM) for operand in operands])


def pairs_of(size, shift, stride=1):
    members = size // stride
    xor = members & (members - 1) == 0
    pairs = []
    for source in range(size):
        unit, rest = divmod(source, stride)
        target = unit ^ shift if xor else (unit + shift) % members
        pairs.append((source, target * stride + rest))
    return pairs


def exchange(value, axis, stride=1):
    size = lax.axis_size(axis)
    pieces = []
    for shift in range(1, size // stride):
        pieces.append(lax.ppermute(value, axis, pairs_of(size, shift, stride)))
    return pieces


def dot(left, right):
    return jnp.dot(left, right, preferred_element_type=F32)


def forward_kernel(half_rows, gathered, inverse, couple, keep, give, rhs):
    slabs, row_count, _ = gathered.shape
    interior = inverse.shape[0]
    order = [slab for core in range(CORES) for slab in range(core, slabs, CORES)]
    for place, slab in enumerate(order):
        rhs[place * row_count : (place + 1) * row_count, :] = gathered[slab, :, :interior]
    step = dot(rhs[...], inverse[...]).astype(BF16)
    part = dot(step, couple[...]).astype(BF16)
    core = lax.rem(lax.axis_index("col"), CORES)

    @pl.when(core == 0)
    def _():
        keep[...] = part[:half_rows]
        give[...] = part[half_rows:]

    @pl.when(core == 1)
    def _():
        keep[...] = part[half_rows:]
        give[...] = part[:half_rows]


def join_kernel(local, interface, out, sems):
    interior = local.shape[1]
    first = pltpu.make_async_copy(local, out.at[:, :interior], sems.at[0])
    second = pltpu.make_async_copy(interface, out.at[:, interior:], sems.at[1])
    first.start()
    second.start()
    first.wait()
    second.wait()


def add_kernel(*refs):
    out = refs[-1]
    total = refs[0][...].astype(F32)
    for ref in refs[1:-1]:
        total = total + ref[...].astype(F32)
    out[...] = total.astype(BF16)


def pack_kernel(*refs):
    ids, out = refs[-2], refs[-1]
    width = refs[0].shape[1]
    total = refs[0][...].astype(F32)
    for ref in refs[1:-2]:
        total = total + ref[...].astype(F32)
    out[:, :width] = total.astype(BF16)
    out[:, width:] = jnp.broadcast_to(ids[...].astype(F32), (out.shape[0], LANES)).astype(BF16)


def place_kernel(block_count, block_size, gathered, *refs):
    pieces, out = refs[:-1], refs[-1]
    row_count = gathered.shape[1]
    rows, width = out.shape
    interior = gathered.shape[2] - width
    core = lax.rem(lax.axis_index("col"), CORES)
    base = (lax.axis_index("dom") * (width // block_size)).astype(F32)
    span = block_count * block_size
    ids = []
    for piece in pieces:
        tail = piece[:, span:].astype(F32) - base
        for block in range(block_count):
            ids.append(jnp.broadcast_to(tail[:, block : block + 1], (rows, block_size)))
    for target in range(width // block_size):
        lanes = slice(target * block_size, (target + 1) * block_size)
        total = jnp.zeros((rows, block_size), F32)
        for index, name in enumerate(ids):
            piece, block = divmod(index, block_count)
            held = pieces[piece][:, block * block_size : (block + 1) * block_size]
            total = total + jnp.where(name == float(target), held.astype(F32), 0.0)
        source = slice(interior + lanes.start, interior + lanes.stop)
        for chip in range(rows // row_count):
            part = slice(chip * row_count, (chip + 1) * row_count)
            have = gathered[CORES * chip + core, :, source].astype(F32)
            out[part, lanes] = (have - total[part]).astype(BF16)


def interface_kernel(mine, other, inverse, out, reduced):
    core = lax.rem(lax.axis_index("col"), CORES)
    rows = mine.shape[0]

    @pl.when(core == 0)
    def _():
        reduced[:rows] = mine[...]
        reduced[rows:] = other[...]

    @pl.when(core == 1)
    def _():
        reduced[:rows] = other[...]
        reduced[rows:] = mine[...]

    out[...] = dot(reduced[...], inverse[...]).astype(BF16)


def backward_kernel(block_size, ids, total, gathered, couple, out, picked):
    slabs, rows, columns = total.shape
    row_count = gathered.shape[1]
    own_columns = couple.shape[0]
    block_count = couple.shape[1] // block_size
    per_slab = columns // block_size
    col = lax.axis_index("col")
    for block in range(block_count):
        name = ids[0, block]
        slab = lax.div(name, per_slab)
        offset = pl.multiple_of(lax.rem(name, per_slab) * block_size, block_size)
        picked[:, block * block_size : (block + 1) * block_size] = total[slab, :, pl.ds(offset, block_size)]
    row = lax.broadcasted_iota(jnp.int32, (rows, rows), 0)
    place = lax.broadcasted_iota(jnp.int32, (rows, rows), 1)
    owner = lax.div(row, row_count)
    held = (
        lax.rem(owner, CORES) * (rows // CORES)
        + lax.div(owner, CORES) * row_count
        + lax.rem(row, row_count)
    )
    turn = (held == place).astype(F32).astype(BF16)
    local = dot(turn, picked[...]).astype(BF16)
    correction = lax.dot_general(
        local, couple[...], (((1,), (1,)), ((), ())), preferred_element_type=F32
    )
    start = pl.multiple_of(col * own_columns, LANES)
    for slab in range(slabs):
        part = slice(slab * row_count, (slab + 1) * row_count)
        have = gathered[slab, :, pl.ds(start, own_columns)].astype(F32)
        out[part] = (have - correction[part]).astype(BF16)


def stack_kernel(*refs):
    out = refs[-1]
    for index, ref in enumerate(refs[:-1]):
        out[index] = ref[...]


def unit_from(unit, shift, members):
    if members & (members - 1) == 0:
        return lax.bitwise_xor(unit, shift)
    return lax.rem(unit + members - shift, members)


def product_kernel(members, sources, inverse, carry, *refs):
    out = refs[-1]
    columns = refs[0].shape[-1]
    col = lax.axis_index("col")
    unit, core = lax.div(col, CORES), lax.rem(col, CORES)
    total = None if carry is None else carry[...]
    blocks = [ref for ref in refs[:-1] if len(ref.shape) == 2]
    for ref in refs[:-1]:
        if len(ref.shape) == 3:
            blocks += [ref.at[index] for index in range(ref.shape[0])]
    for block, (shift, other) in zip(blocks, sources):
        owner = unit_from(unit, shift, members) * CORES + lax.rem(core + other, CORES)
        start = pl.multiple_of(owner * columns, LANES)
        term = dot(block[...], inverse[pl.ds(start, columns), :])
        total = term if total is None else total + term
    out[...] = total.astype(out.dtype)


def product(members, sources, inverse, carry, blocks, dtype):
    rows, columns = blocks[0].shape[-2:]
    operands = [inverse] + ([] if carry is None else [carry]) + list(blocks)
    kernel = functools.partial(product_kernel, members, sources)
    if carry is None:
        kernel = lambda inverse_ref, *refs: product_kernel(members, sources, inverse_ref, None, *refs)
    return pl.pallas_call(
        kernel,
        out_shape=jax.ShapeDtypeStruct((rows, inverse.shape[1]), dtype),
        in_specs=[WHOLE] * len(operands),
        out_specs=WHOLE,
        compiler_params=pltpu.CompilerParams(vmem_limit_bytes=8 * 2**20),
        cost_estimate=pl.CostEstimate(
            flops=2 * rows * columns * inverse.shape[1] * len(sources),
            bytes_accessed=2**20,
            transcendentals=0,
        ),
    )(*[pltpu.with_memory_space_constraint(operand, pltpu.VMEM) for operand in operands])


def pick_kernel(row_count, total, solution):
    slabs, rows, columns = total.shape
    col = lax.axis_index("col")
    first = lax.rem(col, CORES) * (rows // CORES) + lax.div(col, CORES) * row_count
    pick_row = lax.broadcasted_iota(jnp.int32, (8, rows), 0)
    pick_place = lax.broadcasted_iota(jnp.int32, (8, rows), 1)
    pick = (pick_row + first == pick_place).astype(F32).astype(BF16)
    for slab in range(slabs):
        chosen = dot(pick, total[slab])[:row_count]
        solution[:, slab * columns : (slab + 1) * columns] = chosen.astype(BF16)


def per_device(rhs_interior, interior_inv, coupling, rhs_interface, block_ids, interface_inv):
    rhs_local = rhs_interior[0]
    inverse = interior_inv[0]
    couple = coupling[0]
    row_count, interior = rhs_local.shape
    own_columns, local_count = couple.shape
    block_count = block_ids.shape[1]
    block_size = local_count // block_count
    col_size = lax.axis_size("col")
    rows = row_count * col_size
    half = rows // CORES
    width = rhs_interface.shape[1]
    columns = interface_inv.shape[1]

    joined = pl.pallas_call(
        join_kernel,
        out_shape=jax.ShapeDtypeStruct((row_count, interior + width), BF16),
        in_specs=[pl.BlockSpec(memory_space=pltpu.HBM)] * 2,
        out_specs=WHOLE,
        scratch_shapes=[pltpu.SemaphoreType.DMA((2,))],
        compiler_params=pltpu.CompilerParams(vmem_limit_bytes=8 * 2**20),
        cost_estimate=pl.CostEstimate(
            flops=64 * rows * columns * interior, bytes_accessed=2**20, transcendentals=0
        ),
    )(
        pltpu.with_memory_space_constraint(rhs_local, pltpu.HBM),
        pltpu.with_memory_space_constraint(rhs_interface, pltpu.HBM),
    )
    gathered = lax.all_gather(joined, "col", axis=0)
    ids_row = jnp.pad(block_ids, ((0, 0), (0, LANES - block_count)))

    core_pairs = [(source, source ^ 1) for source in range(col_size)]
    keep, give = run(
        functools.partial(forward_kernel, half),
        [(half, local_count)] * 2,
        [gathered, inverse, couple],
        2 * rows * own_columns * (interior + local_count),
        [pltpu.VMEM((rows, interior), BF16)],
        limit=12,
    )
    other = lax.ppermute(give, "col", core_pairs)
    (pair,) = run(add_kernel, [(half, local_count)], [keep, other], half * local_count)
    (packed,) = run(
        pack_kernel,
        [(half, local_count + LANES)],
        [pair, *exchange(pair, "col", CORES), ids_row],
        half * local_count,
    )
    (reduced,) = run(
        functools.partial(place_kernel, block_count, block_size),
        [(half, width)],
        [gathered, packed, *exchange(packed, "dom")],
        rows * width * 64,
        limit=16,
    )
    reduced_other = lax.ppermute(reduced, "col", core_pairs)
    (part_solution,) = run(
        interface_kernel,
        [(rows, columns)],
        [reduced, reduced_other, interface_inv],
        2 * rows * width * columns,
        [pltpu.VMEM((rows, width), BF16)],
    )
    (total,) = run(
        add_kernel,
        [(rows, columns)],
        [part_solution, *exchange(part_solution, "dom")],
        rows * columns,
    )
    every_total = lax.all_gather(total, "col", axis=0)
    interior_rhs = pl.pallas_call(
        functools.partial(backward_kernel, block_size),
        out_shape=jax.ShapeDtypeStruct((rows, own_columns), BF16),
        in_specs=[pl.BlockSpec(memory_space=pltpu.SMEM)] + [WHOLE] * 3,
        out_specs=WHOLE,
        scratch_shapes=[pltpu.VMEM((rows, local_count), BF16)],
        compiler_params=pltpu.CompilerParams(vmem_limit_bytes=8 * 2**20),
        cost_estimate=pl.CostEstimate(
            flops=2 * rows * own_columns * local_count, bytes_accessed=2**20, transcendentals=0
        ),
    )(
        block_ids,
        pltpu.with_memory_space_constraint(every_total, pltpu.VMEM),
        pltpu.with_memory_space_constraint(gathered, pltpu.VMEM),
        pltpu.with_memory_space_constraint(couple, pltpu.VMEM),
    )
    members = col_size // CORES
    far = exchange(interior_rhs, "col", CORES)
    peer = lax.ppermute(interior_rhs, "col", core_pairs)
    (solution,) = run(
        functools.partial(pick_kernel, row_count),
        [(row_count, columns * col_size)],
        [every_total],
        2 * 8 * rows * columns * col_size,
    )
    near = [interior_rhs, peer]
    first_sum = product(members, [(0, 0), (0, 1)], inverse, None, near, F32)
    (stacked,) = run(stack_kernel, [(members - 1, rows, own_columns)], far, rows * own_columns)
    far_peer = lax.ppermute(stacked, "col", core_pairs)
    shifts = range(1, members)
    second_sum = product(members, [(k, 0) for k in shifts], inverse, first_sum, [stacked], F32)
    result = product(members, [(k, 1) for k in shifts], inverse, second_sum, [far_peer], BF16)
    return (result[None], solution)


def solution(mesh):
    placed = (
        P("dom", "col", None),
        P("dom", None, "col"),
        P("dom", "col", None),
        P("col", "dom"),
        P("dom", None),
        P("dom", "col"),
    )
    return jax.shard_map(
        per_device,
        mesh=mesh,
        in_specs=placed,
        out_specs=(P("dom", None, "col"), P("col", None)),
        check_vma=False,
    )
```

```python
import functools

import jax
import jax.numpy as jnp
from jax import lax
from jax.experimental import pallas as pl
from jax.experimental.pallas import tpu as pltpu
from jax.sharding import PartitionSpec as P


LANES = 128
CORES = 2
BF16 = jnp.bfloat16
F32 = jnp.float32
WHOLE = pl.BlockSpec(memory_space=pltpu.VMEM)


def run(kernel, outputs, operands, flops, scratch=(), limit=8):
    return pl.pallas_call(
        kernel,
        out_shape=[jax.ShapeDtypeStruct(shape, BF16) for shape in outputs],
        in_specs=[WHOLE] * len(operands),
        out_specs=[WHOLE] * len(outputs),
        scratch_shapes=list(scratch),
        compiler_params=pltpu.CompilerParams(vmem_limit_bytes=limit * 2**20),
        cost_estimate=pl.CostEstimate(flops=flops, bytes_accessed=2**20, transcendentals=0),
    )(*[pltpu.with_memory_space_constraint(operand, pltpu.VMEM) for operand in operands])


def pairs_of(size, shift, stride):
    members = size // stride
    xor = members & (members - 1) == 0
    pairs = []
    for unit in range(members):
        target = unit ^ shift if xor else (unit + shift) % members
        pairs += [(unit * stride + lane, target * stride + lane) for lane in range(stride)]
    return pairs


def exchange(value, axis, stride=1):
    size = lax.axis_size(axis)
    pieces = []
    for shift in range(1, size // stride):
        pieces.append(lax.ppermute(value, axis, pairs_of(size, shift, stride)))
    return pieces


def dot(left, right):
    return jnp.dot(left, right, preferred_element_type=F32)


def forward_kernel(gathered, inverse, couple, keep, give, rhs):
    slabs, row_count, _ = gathered.shape
    interior = inverse.shape[0]
    for slab in range(slabs):
        rhs[slab * row_count : (slab + 1) * row_count, :] = gathered[slab, :, :interior]
    step = dot(rhs[...], inverse[...]).astype(BF16)
    part = dot(step, couple[...]).astype(BF16)
    half = keep.shape[0]
    core = lax.rem(lax.axis_index("col"), CORES)

    @pl.when(core == 0)
    def _():
        keep[...] = part[:half]
        give[...] = part[half:]

    @pl.when(core == 1)
    def _():
        keep[...] = part[half:]
        give[...] = part[:half]


def join_kernel(local, interface, out, sems):
    interior = local.shape[1]
    first = pltpu.make_async_copy(local, out.at[:, :interior], sems.at[0])
    second = pltpu.make_async_copy(interface, out.at[:, interior:], sems.at[1])
    first.start()
    second.start()
    first.wait()
    second.wait()


def add_kernel(*refs):
    out = refs[-1]
    total = refs[0][...].astype(F32)
    for ref in refs[1:-1]:
        total = total + ref[...].astype(F32)
    out[...] = total.astype(BF16)


def pack_kernel(*refs):
    ids, out = refs[-2], refs[-1]
    width = refs[0].shape[1]
    total = refs[0][...].astype(F32)
    for ref in refs[1:-2]:
        total = total + ref[...].astype(F32)
    out[:, :width] = total.astype(BF16)
    out[:, width:] = jnp.broadcast_to(ids[...].astype(F32), (out.shape[0], LANES)).astype(BF16)


def rows_kernel(gathered, interface_rows, own):
    slabs, row_count, total = gathered.shape
    interior = total - interface_rows.shape[1]
    own_columns = own.shape[1]
    col = lax.axis_index("col")
    start = pl.multiple_of(col * own_columns, LANES)
    half = slabs // CORES
    base = lax.rem(col, CORES) * half
    for slab in range(slabs):
        part = slice(slab * row_count, (slab + 1) * row_count)
        own[part] = gathered[slab, :, pl.ds(start, own_columns)]
        if slab < half:
            interface_rows[part] = gathered[base + slab, :, interior:]


def turn_kernel(couple, out):
    out[...] = couple[...].T


def place_kernel(block_count, block_size, interface_rows, *refs):
    pieces, out = refs[:-1], refs[-1]
    rows, width = out.shape
    targets = width // block_size
    base = (lax.axis_index("dom") * targets).astype(F32)
    span = block_count * block_size
    tile = 8
    names = []
    for piece in pieces:
        tail = piece[:tile, span:].astype(F32) - base
        for block in range(block_count):
            names.append(jnp.broadcast_to(tail[:, block : block + 1], (tile, block_size)))
    for target in range(targets):
        lanes = slice(target * block_size, (target + 1) * block_size)
        have = [
            interface_rows[row : row + tile, lanes].astype(F32) for row in range(0, rows, tile)
        ]
        for index, name in enumerate(names):
            piece, block = divmod(index, block_count)
            source = slice(block * block_size, (block + 1) * block_size)
            here = name == float(target)
            for row in range(0, rows, tile):
                held = pieces[piece][row : row + tile, source].astype(F32)
                have[row // tile] -= jnp.where(here, held, 0.0)
        out[:, lanes] = jnp.concatenate(have, axis=0).astype(BF16)


def interface_kernel(mine, other, inverse, out, reduced):
    core = lax.rem(lax.axis_index("col"), CORES)
    half = mine.shape[0]

    @pl.when(core == 0)
    def _():
        reduced[:half] = mine[...]
        reduced[half:] = other[...]

    @pl.when(core == 1)
    def _():
        reduced[:half] = other[...]
        reduced[half:] = mine[...]

    out[...] = dot(reduced[...], inverse[...]).astype(BF16)


def backward_kernel(block_size, ids, total, own, couple_turned, out, picked):
    columns = total.shape[2]
    block_count = couple_turned.shape[0] // block_size
    per_slab = columns // block_size
    for block in range(block_count):
        name = ids[0, block]
        slab = lax.div(name, per_slab)
        offset = pl.multiple_of(lax.rem(name, per_slab) * block_size, block_size)
        picked[:, block * block_size : (block + 1) * block_size] = total[slab, :, pl.ds(offset, block_size)]
    correction = dot(picked[...], couple_turned[...])
    out[...] = (own[...].astype(F32) - correction).astype(BF16)


def stack_kernel(*refs):
    out = refs[-1]
    for index, ref in enumerate(refs[:-1]):
        out[index] = ref[...]


def unit_from(unit, shift, members):
    if members & (members - 1) == 0:
        return lax.bitwise_xor(unit, shift)
    return lax.rem(unit + members - shift, members)


def product_kernel(members, sources, inverse, carry, *refs):
    out = refs[-1]
    columns = refs[0].shape[-1]
    col = lax.axis_index("col")
    unit, core = lax.div(col, CORES), lax.rem(col, CORES)
    total = None if carry is None else carry[...]
    blocks = [ref for ref in refs[:-1] if len(ref.shape) == 2]
    for ref in refs[:-1]:
        if len(ref.shape) == 3:
            blocks += [ref.at[index] for index in range(ref.shape[0])]
    for block, (shift, other) in zip(blocks, sources):
        owner = unit_from(unit, shift, members) * CORES + lax.rem(core + other, CORES)
        start = pl.multiple_of(owner * columns, LANES)
        term = dot(block[...], inverse[pl.ds(start, columns), :])
        total = term if total is None else total + term
    out[...] = total.astype(out.dtype)


def product(members, sources, inverse, carry, blocks, dtype):
    rows, columns = blocks[0].shape[-2:]
    operands = [inverse] + ([] if carry is None else [carry]) + list(blocks)
    kernel = functools.partial(product_kernel, members, sources)
    if carry is None:
        kernel = lambda inverse_ref, *refs: product_kernel(members, sources, inverse_ref, None, *refs)
    return pl.pallas_call(
        kernel,
        out_shape=jax.ShapeDtypeStruct((rows, inverse.shape[1]), dtype),
        in_specs=[WHOLE] * len(operands),
        out_specs=WHOLE,
        compiler_params=pltpu.CompilerParams(vmem_limit_bytes=8 * 2**20),
        cost_estimate=pl.CostEstimate(
            flops=2 * rows * columns * inverse.shape[1] * len(sources),
            bytes_accessed=2**20,
            transcendentals=0,
        ),
    )(*[pltpu.with_memory_space_constraint(operand, pltpu.VMEM) for operand in operands])


def pick_kernel(row_count, total, solution):
    slabs, rows, columns = total.shape
    col = lax.axis_index("col")
    first = col * row_count
    pick_row = lax.broadcasted_iota(jnp.int32, (8, rows), 0)
    pick_place = lax.broadcasted_iota(jnp.int32, (8, rows), 1)
    pick = (pick_row + first == pick_place).astype(F32).astype(BF16)
    for slab in range(slabs):
        chosen = dot(pick, total[slab])[:row_count]
        solution[:, slab * columns : (slab + 1) * columns] = chosen.astype(BF16)


def per_device(rhs_interior, interior_inv, coupling, rhs_interface, block_ids, interface_inv):
    rhs_local = rhs_interior[0]
    inverse = interior_inv[0]
    couple = coupling[0]
    row_count, interior = rhs_local.shape
    own_columns, local_count = couple.shape
    block_count = block_ids.shape[1]
    block_size = local_count // block_count
    col_size = lax.axis_size("col")
    rows = row_count * col_size
    width = rhs_interface.shape[1]
    columns = interface_inv.shape[1]

    joined = pl.pallas_call(
        join_kernel,
        out_shape=jax.ShapeDtypeStruct((row_count, interior + width), BF16),
        in_specs=[pl.BlockSpec(memory_space=pltpu.HBM)] * 2,
        out_specs=WHOLE,
        scratch_shapes=[pltpu.SemaphoreType.DMA((2,))],
        compiler_params=pltpu.CompilerParams(vmem_limit_bytes=8 * 2**20),
        cost_estimate=pl.CostEstimate(
            flops=64 * rows * columns * interior, bytes_accessed=2**20, transcendentals=0
        ),
    )(
        pltpu.with_memory_space_constraint(rhs_local, pltpu.HBM),
        pltpu.with_memory_space_constraint(rhs_interface, pltpu.HBM),
    )
    gathered = lax.all_gather(joined, "col", axis=0)
    ids_row = jnp.pad(block_ids, ((0, 0), (0, LANES - block_count)))

    core_pairs = [(source, source ^ 1) for source in range(col_size)]
    half = rows // CORES
    keep, give = run(
        forward_kernel,
        [(half, local_count)] * 2,
        [gathered, inverse, couple],
        2 * rows * own_columns * (interior + local_count),
        [pltpu.VMEM((rows, interior), BF16)],
        limit=12,
    )
    other = lax.ppermute(give, "col", core_pairs)
    (pair,) = run(add_kernel, [(half, local_count)], [keep, other], half * local_count)
    plane = exchange(pair, "col", CORES)
    interface_rows, own_rhs = run(
        rows_kernel, [(half, width), (rows, own_columns)], [gathered], rows * width
    )
    (packed,) = run(
        pack_kernel,
        [(half, local_count + LANES)],
        [pair, *plane, ids_row],
        half * local_count,
    )
    (reduced,) = run(
        functools.partial(place_kernel, block_count, block_size),
        [(half, width)],
        [interface_rows, packed, *exchange(packed, "dom")],
        half * width * 64,
        limit=16,
    )
    reduced_other = lax.ppermute(reduced, "col", core_pairs)
    (part_solution,) = run(
        interface_kernel,
        [(rows, columns)],
        [reduced, reduced_other, interface_inv],
        2 * rows * width * columns,
        [pltpu.VMEM((rows, width), BF16)],
    )
    folds = exchange(part_solution, "dom")
    (couple_turned,) = run(
        turn_kernel, [(local_count, own_columns)], [couple], own_columns * local_count
    )
    (total,) = run(
        add_kernel, [(rows, columns)], [part_solution, *folds], rows * columns
    )
    every_total = lax.all_gather(total, "col", axis=0)
    interior_rhs = pl.pallas_call(
        functools.partial(backward_kernel, block_size),
        out_shape=jax.ShapeDtypeStruct((rows, own_columns), BF16),
        in_specs=[pl.BlockSpec(memory_space=pltpu.SMEM)] + [WHOLE] * 3,
        out_specs=WHOLE,
        scratch_shapes=[pltpu.VMEM((rows, local_count), BF16)],
        compiler_params=pltpu.CompilerParams(vmem_limit_bytes=8 * 2**20),
        cost_estimate=pl.CostEstimate(
            flops=2 * rows * own_columns * local_count, bytes_accessed=2**20, transcendentals=0
        ),
    )(
        block_ids,
        pltpu.with_memory_space_constraint(every_total, pltpu.VMEM),
        pltpu.with_memory_space_constraint(own_rhs, pltpu.VMEM),
        pltpu.with_memory_space_constraint(couple_turned, pltpu.VMEM),
    )
    members = col_size // CORES
    far = exchange(interior_rhs, "col", CORES)
    peer = lax.ppermute(interior_rhs, "col", core_pairs)
    (solution,) = run(
        functools.partial(pick_kernel, row_count),
        [(row_count, columns * col_size)],
        [every_total],
        2 * 8 * rows * columns * col_size,
    )
    near = [interior_rhs, peer]
    first_sum = product(members, [(0, 0), (0, 1)], inverse, None, near, F32)
    (stacked,) = run(stack_kernel, [(members - 1, rows, own_columns)], far, rows * own_columns)
    far_peer = lax.ppermute(stacked, "col", core_pairs)
    shifts = range(1, members)
    second_sum = product(members, [(k, 0) for k in shifts], inverse, first_sum, [stacked], F32)
    result = product(members, [(k, 1) for k in shifts], inverse, second_sum, [far_peer], BF16)
    return (result[None], solution)


def solution(mesh):
    placed = (
        P("dom", "col", None),
        P("dom", None, "col"),
        P("dom", "col", None),
        P("col", "dom"),
        P("dom", None),
        P("dom", "col"),
    )
    return jax.shard_map(
        per_device,
        mesh=mesh,
        in_specs=placed,
        out_specs=(P("dom", None, "col"), P("col", None)),
        check_vma=False,
    )
```
